32 devices in a mesh: row: 8 (over z, core), col: 4 (over y, x).
Axes of the slice: x: 2, y: 2, z: 4, core: 2. Of those that a mesh axis runs over, the one named last changes fastest.
Arguments:
- matrix: float32 [1728, 65536], P('row', 'col'), may hold values from -6 to 6
- range_basis: float32 [1728, 384], P('col', 'row'), may hold values from -0.21875 to 0.21875
Outputs:
- projected: float32 [384, 65536], P('row')
The draws below stay inside these ranges and needn't reach their ends.
All inputs are finite; a program needn't handle non-finite values.
Results may differ from the reference program's by a relative error of at most 0.000071.
Values sent between devices are 32-bit elements; how exact they have to be, the bound alone decides.
A program may use at most 128 MiB of HBM per device.

```python
import jax
import jax.numpy as jnp
from jax import lax

K = 384
M = 1728
N = 65536


def spiked(entries, own_key, source, target, shards_of, factor):
    owner, partner = [(jnp.arange(entries.shape[axis_at]) // (entries.shape[axis_at] // shards_of)).reshape([-1 if axis == axis_at else 1 for axis in range(entries.ndim)]) for axis_at in (source, target)]
    chosen = jax.random.permutation(own_key, shards_of)[partner]
    strong = (owner == chosen) | (owner == (partner + shards_of // 2) % shards_of)
    return jnp.where(strong, factor * entries, entries)


def levels(rng, shape, pieces, least, high):
    gain = 1.0
    for dim, parts in pieces:
        draws = jax.random.uniform(jax.random.fold_in(jax.random.fold_in(rng, 6), dim), (parts,), jnp.float32, least / len(pieces), high / len(pieces))
        gain = gain * jnp.repeat(jnp.exp(draws), shape[dim] // parts).reshape((-1,) + (1,) * (len(shape) - 1 - dim))
    return gain


def centred(stream_key, dims, width, bound, shards=(), kind=jnp.bfloat16):
    array = width * jax.random.normal(stream_key, dims, jnp.float32)
    if shards:
        array = array * levels(stream_key, dims, shards, -0.22, 0.18)
    return jnp.clip(array, -bound, bound).astype(kind)


def gaussian_with(key, shape, scale, reach, cuts, heavy, dtype=jnp.bfloat16):
    result = scale * jax.random.normal(key, shape, jnp.float32)
    if cuts:
        result = result * levels(key, shape, cuts, -0.22, 0.18)
    return jnp.clip(spiked(result, jax.random.fold_in(key, 3), *heavy), -reach, reach).astype(dtype)


def setup_inputs(seed: int = 0) -> dict:
    arg_keys = jax.random.split(jax.random.key(seed), 3)
    matrix = centred(arg_keys[0], (M, N), 1.0, 6.0, ((0, 8), (1, 4)), jnp.float32)
    range_basis = gaussian_with(arg_keys[1], (M, K), M ** -0.5, 0.21875, ((0, 4), (1, 8)), (0, 1, 8, 2.0), jnp.float32)
    return {"matrix": matrix, "range_basis": range_basis}


def reference(matrix, range_basis):
    return lax.dot_general(range_basis, matrix, (((0,), (0,)), ((), ())), precision=lax.Precision.HIGHEST, preferred_element_type=jnp.float32)
```

```python
import jax
import jax.numpy as jnp
from jax import lax
from jax.experimental import pallas as pl
from jax.experimental.pallas import tpu as pltpu
from jax.sharding import PartitionSpec as P

MESH = pl.DeviceIdType.MESH
CHUNKS = 16
CORES = 2


def split_parts(value):
    high = value.astype(jnp.bfloat16)
    return high, (value - high.astype(jnp.float32)).astype(jnp.bfloat16)


def kernel(
    chips, cols, basis_ref, matrix_ref, out_ref, basis, halves, rows, part, sums,
    basis_send, basis_recv, rows_local, rows_send, rows_recv, sum_send, sum_recv, out_send, out_recv,
):
    row, col = lax.axis_index("row"), lax.axis_index("col")
    chip, core = row // CORES, row % CORES
    vectors = basis_ref.shape[0]
    depth = matrix_ref.shape[0]
    chunks, _, width = rows.shape
    block = matrix_ref.shape[1]

    def basis_copy(target):
        return pltpu.make_async_remote_copy(
            src_ref=basis_ref,
            dst_ref=basis.at[pl.ds(chip * vectors, vectors)],
            send_sem=basis_send.at[target],
            recv_sem=basis_recv.at[chip],
            device_id={"row": CORES * col + core, "col": target},
            device_id_type=MESH,
        )

    def basis_own():
        return pltpu.make_async_copy(
            basis_ref, basis.at[pl.ds(chip * vectors, vectors)], basis_recv.at[chip]
        )

    def rows_own(step):
        return pltpu.make_async_copy(
            matrix_ref.at[:, pl.ds(step * width, width)],
            rows.at[step, pl.ds(core * depth, depth)],
            rows_local.at[step],
        )

    def rows_peer(step, owner):
        return pltpu.make_async_remote_copy(
            src_ref=matrix_ref.at[:, pl.ds(step * width, width)],
            dst_ref=rows.at[step, pl.ds(owner * depth, depth)],
            send_sem=rows_send.at[step],
            recv_sem=rows_recv.at[step],
            device_id={"row": CORES * chip + 1 - core, "col": col},
            device_id_type=MESH,
        )

    def sum_copy(source, owner, slot, step, towards):
        return pltpu.make_async_remote_copy(
            src_ref=source,
            dst_ref=sums.at[slot, step],
            send_sem=sum_send.at[owner, step],
            recv_sem=sum_recv.at[slot, step],
            device_id={"row": CORES * towards + core, "col": col},
            device_id_type=MESH,
        )

    def part_of(step, owner):
        return part.at[step, pl.ds(owner * vectors, vectors)]

    def send_up(source, owner, step):
        sum_copy(source, owner, owner, step, chip + 1).start()

    def send_down(source, owner, step):
        slot = jnp.where(owner == chip - 1, chips, owner)
        sum_copy(source, owner, slot, step, chip - 1).start()

    def sum_wait(slot, step):
        neighbour = jnp.where(chip == 0, 1, chip - 1)
        sum_copy(sums.at[slot, step], 0, slot, step, neighbour).wait_recv()

    def out_at(step, owner):
        return out_ref.at[:, pl.ds(owner * block + step * width, width)]

    def out_copy(step, target):
        return pltpu.make_async_remote_copy(
            src_ref=part_of(step, chip),
            dst_ref=out_at(step, col),
            send_sem=out_send.at[target, step],
            recv_sem=out_recv.at[col, step],
            device_id={"row": row, "col": target},
            device_id_type=MESH,
        )

    def out_wait(step, source):
        pltpu.make_async_remote_copy(
            src_ref=part_of(step, chip),
            dst_ref=out_at(step, source),
            send_sem=out_send.at[source, step],
            recv_sem=out_recv.at[source, step],
            device_id={"row": row, "col": source},
            device_id_type=MESH,
        ).wait_recv()

    def out_own(step):
        return pltpu.make_async_copy(part_of(step, chip), out_at(step, col), out_recv.at[col, step])

    for shift in range(cols):
        target = lax.rem(col + shift, cols)
        if shift:
            basis_copy(target).start()
        else:
            pl.when(chip == col)(lambda: basis_own().start())
            pl.when(chip != col)(lambda: basis_copy(col).start())

    @pl.loop(0, chunks)
    def _(step):
        rows_peer(step, core).start()
        rows_own(step).start()

    for source in range(chips):
        pltpu.make_async_copy(
            basis_ref, basis.at[pl.ds(source * vectors, vectors)], basis_recv.at[source]
        ).wait()
    high, low = split_parts(basis[...])
    count = chips * vectors
    halves[:count] = high
    halves[count:] = low

    tile = min(256, width)

    @pl.loop(0, chunks)
    def _(step):
        rows_own(step).wait()
        rows_peer(step, 1 - core).wait_recv()

        @pl.loop(0, width // tile)
        def _(at):
            lanes = pl.ds(pl.multiple_of(at * tile, tile), tile)
            right, rest = split_parts(rows[step, :, lanes])
            inner = CORES * depth
            both = jnp.dot(halves[:, :inner], right, preferred_element_type=jnp.float32)
            third = jnp.dot(halves[:count, :inner], rest, preferred_element_type=jnp.float32)
            part[step, :, lanes] = both[:count] + (both[count:] + third)

        @pl.when(chip == 0)
        def _():
            for owner in range(chips - 1, 0, -1):
                send_up(part_of(step, owner), owner, step)

        @pl.when(chip == chips - 1)
        def _():
            for owner in range(chips - 1):
                send_down(part_of(step, owner), owner, step)

    def add(step, slot, owner):
        at = pl.ds(pl.multiple_of(owner * vectors, vectors), vectors)
        return sums[slot, step] + part[step, at]

    @pl.loop(0, chunks)
    def _(step):
        for owner in range(chips - 1, 0, -1):

            @pl.when((chip > 0) & (chip < owner))
            def _():
                sum_wait(owner, step)
                sums[owner, step] = add(step, owner, owner)
                send_up(sums.at[owner, step], owner, step)

            down = chips - 1 - owner

            @pl.when((chip < chips - 1) & (chip > down))
            def _():
                sum_wait(down, step)
                sums[down, step] = add(step, down, down)
                send_down(sums.at[down, step], down, step)

        mine = pl.ds(pl.multiple_of(chip * vectors, vectors), vectors)

        @pl.when(chip > 0)
        def _():
            sum_wait(chip, step)
            part[step, mine] = sums[chip, step] + part[step, mine]

        @pl.when(chip < chips - 1)
        def _():
            sum_wait(chips, step)
            part[step, mine] = sums[chips, step] + part[step, mine]

        for shift in range(1, cols):
            out_copy(step, lax.rem(col + shift, cols)).start()
        out_own(step).start()

    for shift in range(cols):
        target = lax.rem(col + shift, cols)
        if shift:
            basis_copy(target).wait_send()
        else:
            pl.when(chip != col)(lambda: basis_copy(col).wait_send())

    @pl.loop(0, chunks)
    def _(step):
        rows_peer(step, core).wait_send()
        for owner in range(chips):
            neighbour = jnp.where(chip == 0, 1, chip - 1)

            @pl.when(owner != chip)
            def _():
                sum_copy(part_of(step, owner), owner, owner, step, neighbour).wait_send()

        for shift in range(1, cols):
            other = lax.rem(col + shift, cols)
            out_copy(step, other).wait_send()
            out_wait(step, other)
        out_own(step).wait()


def solution(mesh):
    chips, cols = mesh.shape["row"] // CORES, mesh.shape["col"]

    def per_device(matrix, range_basis):
        depth, block = matrix.shape
        inner, vectors = range_basis.shape
        assert chips == cols and inner == CORES * depth
        padded = -(-inner // 128) * 128
        width = block // CHUNKS
        mine = jnp.pad(range_basis.T, ((0, 0), (0, padded - inner)))
        count = chips * vectors
        dma = pltpu.SemaphoreType.DMA
        return pl.pallas_call(
            lambda *refs: kernel(chips, cols, *refs),
            out_shape=jax.ShapeDtypeStruct((vectors, cols * block), jnp.float32),
            in_specs=[
                pl.BlockSpec(memory_space=pltpu.VMEM),
                pl.BlockSpec(memory_space=pl.ANY),
            ],
            out_specs=pl.BlockSpec(memory_space=pl.ANY),
            scratch_shapes=[
                pltpu.VMEM((count, padded), jnp.float32),
                pltpu.VMEM((2 * count, padded), jnp.bfloat16),
                pltpu.VMEM((CHUNKS, inner, width), jnp.float32),
                pltpu.VMEM((CHUNKS, count, width), jnp.float32),
                pltpu.VMEM((chips + 1, CHUNKS, vectors, width), jnp.float32),
                dma((cols,)),
                dma((chips,)),
                dma((CHUNKS,)),
                dma((CHUNKS,)),
                dma((CHUNKS,)),
                dma((chips, CHUNKS)),
                dma((chips + 1, CHUNKS)),
                dma((cols, CHUNKS)),
                dma((cols, CHUNKS)),
            ],
            compiler_params=pltpu.CompilerParams(
                has_side_effects=True, vmem_limit_bytes=66_000_000
            ),
        )(mine, matrix)

    return jax.shard_map(
        per_device,
        mesh=mesh,
        in_specs=(P("row", "col"), P("col", "row")),
        out_specs=P("row", None),
        check_vma=False,
    )
```
